32 devices in a mesh: tm: 4 (over y, x), space: 8 (over z, core).
Axes of the slice: x: 2, y: 2, z: 4, core: 2. Of those that a mesh axis runs over, the one named last changes fastest.
Arguments:
- states: float32 [4, 256, 256, 256], P('tm', 'space'), may hold values from -4 to 4
- forcing: float32 [4, 256, 256, 256], P('tm', 'space'), may hold values from -4 to 4
- inflow: float32 [256, 256, 256], P('space'), may hold values from -4 to 4
- timestep: float32 [1], replicated, may hold values from 0.05 to 0.2
Outputs:
- new_states: float32 [4, 256, 256, 256], P('tm', 'space')
- defects: float32 [4, 256, 256, 256], P('tm', 'space')
The draws below stay inside these ranges and needn't reach their ends.
All inputs are finite; a program needn't handle non-finite values.
Results may differ from the reference program's by a relative error of at most 0.00013.
Values sent between devices are 32-bit elements; how exact they have to be, the bound alone decides.
No kernel may reach another device: no remote copies, remote signals or barrier semaphores. Data moves between devices by JAX's collectives and lax.ppermute only.
A program may use at most 192 MiB of HBM per device.

```python
import math
import jax
import jax.numpy as jnp

GRID = 256
FINE = 8
INTERVALS = 4


def draw_forcing(key, part):
    extents = (INTERVALS, GRID, GRID, GRID)
    jagged = jax.random.normal(key, extents, jnp.float32)
    return jnp.clip(jagged, -4.0, 4.0)


def levels(rng, extent, cuts, smallest, largest):
    gain = 1.0
    for dim, blocks in cuts:
        steps = jax.random.uniform(jax.random.fold_in(jax.random.fold_in(rng, 6), dim), (blocks,), jnp.float32, smallest / len(cuts), largest / len(cuts))
        gain = gain * jnp.repeat(jnp.exp(steps), extent[dim] // blocks).reshape((-1,) + (1,) * (len(extent) - 1 - dim))
    return gain


def gaussian(own_key, extent, scale, most, split=(), kind=jnp.bfloat16):
    drawn = jax.random.normal(own_key, extent, jnp.float32) * scale
    if len(split) > 0:
        drawn = levels(own_key, extent, split, -0.22, 0.18) * drawn
    return jnp.clip(drawn, min=-most, max=most).astype(kind)


def setup_inputs(seed: int = 0) -> dict:
    key_list = jax.random.split(jax.random.key(seed), 5)
    states = gaussian(key_list[0], (INTERVALS, GRID, GRID, GRID), 1.0, 4.0, ((0, 4), (1, 8)), jnp.float32)
    forcing = draw_forcing(jax.random.fold_in(key_list[4], 71), 0)
    inflow = gaussian(key_list[2], (GRID, GRID, GRID), 1.0, 4.0, ((0, 8),), jnp.float32)
    timestep = jnp.clip(jnp.exp(jax.random.uniform(key_list[3], (1,), jnp.float32, math.log(0.05), math.log(0.2))), 0.05, 0.2)
    return dict(states=states, forcing=forcing, inflow=inflow, timestep=timestep)


def symbols(stepsize):
    angles = jnp.arange(GRID, dtype=jnp.float32) * (2.0 * math.pi / GRID)
    lattice = 2.0 - 2.0 * jnp.cos(angles)
    laplace = lattice[:, None, None] + lattice[None, :, None] + lattice[None, None, : GRID // 2 + 1]
    damping = 1.0 / (1.0 + stepsize * laplace)
    coarse = 1.0 / (1.0 + FINE * stepsize * laplace)
    return damping, coarse


def reference(states, forcing, inflow, timestep):
    stepsize = timestep[0]
    damping, coarse = symbols(stepsize)
    spec_states = jnp.fft.rfftn(states, axes=(1, 2, 3))
    spec_forcing = jnp.fft.rfftn(forcing, axes=(1, 2, 3))
    spec_inflow = jnp.fft.rfftn(inflow)

    def advance(spectrum, source):
        for repeat in range(FINE):
            spectrum = damping * (spectrum + stepsize * source)
        return spectrum

    correction = jnp.zeros_like(spec_inflow)
    relaxed = spec_inflow
    defect = jnp.zeros_like(spec_inflow)
    updated_list = []
    defect_list = []
    for interval in range(INTERVALS):
        if interval > 0:
            relaxed = advance(spec_states[interval - 1], spec_forcing[interval - 1])
            correction = coarse * correction + defect
        defect = advance(relaxed, spec_forcing[interval]) - advance(spec_states[interval], spec_forcing[interval])
        updated_list.append(relaxed + correction)
        defect_list.append(defect)
    new_states = jnp.fft.irfftn(jnp.stack(updated_list), s=(GRID, GRID, GRID), axes=(1, 2, 3))
    defects = jnp.fft.irfftn(jnp.stack(defect_list), s=(GRID, GRID, GRID), axes=(1, 2, 3))
    return new_states.astype(jnp.float32), defects.astype(jnp.float32)
```

```python
import math

import jax
import jax.numpy as jnp
from jax import lax
from jax.experimental import pallas as pl
from jax.experimental.pallas import tpu as pltpu
from jax.sharding import Mesh, PartitionSpec as P

FINE = 8
CHUNKS = 4
SUB = 8
LANE = 128
VMEM = 56 * 1024 * 1024


def hartley_table(extent):
    wavenumber = jnp.arange(extent, dtype=jnp.int32)
    product = wavenumber[:, None] * wavenumber[None, :] % extent
    angles = product.astype(jnp.float32) * (2.0 * math.pi / extent)
    return (jnp.cos(angles) + jnp.sin(angles)) * (1.0 / math.sqrt(extent))


def lattice_symbol(wavenumber, extent):
    angles = (wavenumber % extent).astype(jnp.float32) * (2.0 * math.pi / extent)
    return 2.0 - 2.0 * jnp.cos(angles)


def power(base, exponent):
    result = None
    while exponent:
        if exponent & 1:
            result = base if result is None else result * base
        exponent >>= 1
        if exponent:
            base = base * base
    return result


def filter_of(mu, step, order):
    r = 2.0 + mu + 1.0 / step
    z = 2.0 / (r + jnp.sqrt(r * r - 4.0))
    inverse = 1.0 / (1.0 - z * z)
    lead = z / step * inverse
    base = [lead]
    term = lead * (z * z * inverse)
    for _ in range(order - 1):
        base.append(term)
        term = term * inverse
    current = base
    weights = []
    for j in range(1, order + 1):
        if j > 1:
            current = [
                sum((current[i] * base[k - i] for i in range(1, k + 1)), current[0] * base[k])
                for k in range(order)
            ]
        weights.append([current[j - m] for m in range(1, j + 1)])
    return z, weights


def coef_count(intervals):
    rounds = intervals - 2
    return 3 + 2 * FINE + 2 + 3 + rounds * (rounds + 1) // 2 + rounds


def coef_kernel(step_ref, mu_ref, out_ref, *, block, extent, intervals):
    step = step_ref[0]
    mu = mu_ref[...]
    rounds = intervals - 2
    step_v = jnp.zeros_like(mu) + step
    z, weights = filter_of(mu, step_v, FINE)
    prop = weights[FINE - 1]
    gain = [
        step_v * sum((weights[j - 1][m - 1] for j in range(m + 1, FINE + 1)), weights[m - 1][m - 1])
        for m in range(1, FINE + 1)
    ]
    rows = [z, power(z, block), power(z, extent)] + prop + gain
    rows += [sum(prop[1:], prop[0]), sum(gain[1:], gain[0])]
    z, weights = filter_of(mu, FINE * step_v, rounds)
    rows += [z, power(z, block), power(z, extent)]
    for one in weights:
        rows += one
    for one in weights:
        rows.append(sum(one[1:], one[0]))
    for i, row in enumerate(rows):
        out_ref[i] = row


class Coefs:
    def __init__(self, ref, intervals):
        rounds = intervals - 2
        self.z, self.zn, self.zl = ref[0], ref[1], ref[2]
        at = 3
        self.prop = lambda m: ref[2 + m]
        self.gain = lambda m: ref[2 + FINE + m]
        at += 2 * FINE
        self.prop0 = lambda: ref[at]
        self.gain0 = lambda: ref[at + 1]
        at2 = at + 2
        self.coarse_z = lambda: (ref[at2], ref[at2 + 1], ref[at2 + 2])
        at3 = at2 + 3
        self.coarse = lambda j, m: ref[at3 + (j - 1) * j // 2 + m - 1]
        at4 = at3 + rounds * (rounds + 1) // 2
        self.coarse0 = lambda j: ref[at4 + j - 1]


def inflow_state(blocks, zn, zl, block, extent):
    order = len(blocks[0])

    def carried(state, factor, length):
        return [
            factor
            * sum(
                (math.comb(length + i - 1, i) * 1.0 * state[m + i] for i in range(1, order - m)),
                state[m],
            )
            for m in range(order)
        ]

    state = blocks[-1]
    for nearer in blocks[-2::-1]:
        state = [a + b for a, b in zip(nearer, carried(state, zn, block))]
    solved = [None] * order
    closure = 1.0 / (1.0 - zl)
    for m in reversed(range(order)):
        total = state[m]
        for i in range(1, order - m):
            total = total + zl * (math.comb(extent + i - 1, i) * 1.0) * solved[m + i]
        solved[m] = total * closure
    return solved


def sweep(count, body, init, unroll=8):
    unroll = min(unroll, count)

    def group(g, carry):
        for k in range(unroll):
            carry = body(g * unroll + k, carry)
        return carry

    return lax.fori_loop(0, count // unroll, group, init)


def cascade(z, x, states):
    out = []
    for y in states:
        x = z * y + x
        out.append(x)
    return out


def nested(z, inputs, states):
    out = [None] * len(states)
    above = None
    for m in reversed(range(len(states))):
        x = inputs[m] if above is None else inputs[m] + above
        above = z * states[m] + x
        out[m] = above
    return out


def advance_ends_kernel(coef_ref, s_ref, f_ref, out_ref, *, block, extent, intervals):
    c = Coefs(coef_ref, intervals)
    z = c.z
    zero = [jnp.zeros_like(z)] * FINE
    for side in range(2):

        def one(i, carry):
            n = i if side == 0 else block - 1 - i
            return (
                cascade(z, s_ref[0, n], carry[0]),
                cascade(z, f_ref[0, n], carry[1]),
            )

        ys, yf = sweep(block, one, (zero, zero))
        for m in range(FINE):
            out_ref[side, 0, m] = sum(
                (
                    c.prop(m + i + 1) * ys[i] + c.gain(m + i + 1) * yf[i]
                    for i in range(1, FINE - m)
                ),
                c.prop(m + 1) * ys[0] + c.gain(m + 1) * yf[0],
            )


def upstream(place, count, side, d):
    return lax.rem(place + (count - d if side == 0 else d), count)


def ends_of(c, x_ref, out_ref, block):
    z = c.z
    zero = [jnp.zeros_like(z)] * FINE
    for side in range(2):

        def one(i, carry):
            n = i if side == 0 else block - 1 - i
            return cascade(z, x_ref[0, n], carry)

        y = sweep(block, one, zero)
        for m in range(FINE):
            out_ref[side, 0, m] = sum(
                (c.prop(m + i + 1) * y[i] for i in range(1, FINE - m)), c.prop(m + 1) * y[0]
            )


def relax_kernel(
    place_ref, coef_ref, s_ref, f_ref, own_ref, ends_ref, rel_ref, err_ref, out_ref, *, block, extent, intervals
):
    c = Coefs(coef_ref, intervals)
    z = c.z
    count = extent // block
    place = place_ref[0]
    t = pl.program_id(2)

    @pl.when(t == 0)
    def _():
        def one(n, carry):
            value = f_ref[0, n]
            rel_ref[0, n] = value
            err_ref[0, n] = value - own_ref[0, n]
            return carry

        sweep(block, one, 0)

    @pl.when(t > 0)
    def _():
        prop = [c.prop(m + 1) for m in range(FINE)]
        gain = [c.gain(m + 1) for m in range(FINE)]
        for side in range(2):
            start = inflow_state(
                [
                    [ends_ref[upstream(place, count, side, d), side, 0, m] for m in range(FINE)]
                    for d in range(1, count + 1)
                ],
                c.zn,
                c.zl,
                block,
                extent,
            )
            if side == 0:
                prop0, gain0 = c.prop0(), c.gain0()

            def one(i, carry):
                n = i if side == 0 else block - 1 - i
                s = s_ref[0, n]
                f = f_ref[0, n]
                carry = nested(z, [p * s + g * f for p, g in zip(prop, gain)], carry)
                if side == 0:
                    rel_ref[0, n] = carry[0] - (prop0 * s + gain0 * f)
                else:
                    value = rel_ref[0, n] + carry[0]
                    rel_ref[0, n] = value
                    err_ref[0, n] = value - own_ref[0, n]
                return carry

            sweep(block, one, start)

    ends_of(c, err_ref, out_ref, block)


def coarse_inputs(c, d, j):
    return [
        sum(
            (c.coarse(j - 1 - i, m) * d[i] for i in range(1, j - m)),
            c.coarse(j - 1, m) * d[0],
        )
        for m in range(1, j)
    ]


def defect_kernel(
    place_ref, coef_ref, err_ref, ends_ref, def_ref, out_ref, *, block, extent, intervals
):
    c = Coefs(coef_ref, intervals)
    z = c.z
    count = extent // block
    place = place_ref[0]

    def interval(t, carry):
        prop = [c.prop(m + 1) for m in range(FINE)]
        for side in range(2):
            start = inflow_state(
                [
                    [ends_ref[upstream(place, count, side, d), side, t, m] for m in range(FINE)]
                    for d in range(1, count + 1)
                ],
                c.zn,
                c.zl,
                block,
                extent,
            )
            if side == 0:
                prop0 = c.prop0()

            def one(i, carry):
                n = i if side == 0 else block - 1 - i
                x = err_ref[t, n]
                carry = nested(z, [p * x for p in prop], carry)
                if side == 0:
                    def_ref[t, n] = carry[0] - prop0 * x
                else:
                    def_ref[t, n] = def_ref[t, n] + carry[0]
                return carry

            sweep(block, one, start)
        return carry

    lax.fori_loop(0, intervals, interval, 0)
    cz, _, _ = c.coarse_z()
    sizes = [j - 1 for j in range(2, intervals)]
    for side in range(2):

        def one(i, carry):
            n = i if side == 0 else block - 1 - i
            d = [def_ref[t, n] for t in range(intervals - 2)]
            return [
                nested(cz, coarse_inputs(c, d, j), state)
                for j, state in zip(range(2, intervals), carry)
            ]

        ends = sweep(block, one, [[jnp.zeros_like(cz)] * k for k in sizes])
        at = 0
        for state in ends:
            for value in state:
                out_ref[side, at] = value
                at += 1


def correct_kernel(
    place_ref, coef_ref, rel_ref, def_ref, ends_ref, new_ref, *, block, extent, intervals
):
    c = Coefs(coef_ref, intervals)
    count = extent // block
    place = place_ref[0]
    cz, czn, czl = c.coarse_z()
    for side in range(2):
        starts = []
        at = 0
        for j in range(2, intervals):
            starts.append(
                inflow_state(
                    [
                        [ends_ref[upstream(place, count, side, d), side, at + m] for m in range(j - 1)]
                        for d in range(1, count + 1)
                    ],
                    czn,
                    czl,
                    block,
                    extent,
                )
            )
            at += j - 1

        def one(i, carry):
            n = i if side == 0 else block - 1 - i
            d = [def_ref[t, n] for t in range(intervals - 1)]
            carry = [
                nested(cz, coarse_inputs(c, d, j), state)
                for j, state in zip(range(2, intervals), carry)
            ]
            if side == 0:
                new_ref[0, n] = rel_ref[0, n]
                new_ref[1, n] = rel_ref[1, n] + d[0]
            for j, state in zip(range(2, intervals), carry):
                if side == 0:
                    center = sum(
                        (c.coarse0(j - 1 - i) * d[i] for i in range(1, j - 1)),
                        c.coarse0(j - 1) * d[0],
                    )
                    new_ref[j, n] = rel_ref[j, n] + d[j - 1] + (state[0] - center)
                else:
                    new_ref[j, n] = new_ref[j, n] + state[0]
            return carry

        sweep(block, one, starts, 4)


def split(x):
    high = x.astype(jnp.bfloat16)
    return high, (x - high.astype(jnp.float32)).astype(jnp.bfloat16)


def dot3(a, b):
    def dot(x, y):
        return jnp.dot(x, y, preferred_element_type=jnp.float32)

    return dot(a[0], b[0]) + (dot(a[0], b[1]) + dot(a[1], b[0]))


def forward_kernel(*refs, choose, chunks):
    if choose:
        last_ref, x_ref, other_ref, high_ref, low_ref = refs[:5]
        outs = refs[5:]
    else:
        x_ref, high_ref, low_ref = refs[:3]
        outs = refs[3:]
    table = (high_ref[...], low_ref[...])
    planes = x_ref.shape[0]
    for p in range(planes):
        x = x_ref[p]
        if choose:
            x = jnp.where(last_ref[0] > 0, other_ref[p], x)
        y = dot3(table, split(dot3(split(x), table)))
        groups, rows = outs[0].shape[0], outs[0].shape[2]
        y = y.reshape(groups, chunks * rows, y.shape[-1])
        for i, out in enumerate(outs):
            out[:, p] = y[:, i * rows : (i + 1) * rows]


def inverse_kernel(*refs):
    parts, (high_ref, low_ref, out_ref) = refs[:-3], refs[-3:]
    table = (high_ref[...], low_ref[...])
    extent = out_ref.shape[-1]
    for p in range(out_ref.shape[0]):
        x = jnp.concatenate([part[:, p] for part in parts], axis=1).reshape(extent, extent)
        out_ref[p] = dot3(split(dot3(table, split(x))), table)


def on_device(states, forcing, inflow, timestep):
    planes, extent = states.shape[1], states.shape[2]
    intervals = lax.axis_size("tm")
    cores = lax.axis_size("core")
    count = lax.axis_size("line")
    block = planes * cores
    groups = intervals * cores
    rows = extent // groups
    chunks = max(1, min(CHUNKS, rows // SUB))
    part = rows // chunks
    f32 = jnp.float32
    params = lambda n: pltpu.CompilerParams(
        dimension_semantics=("arbitrary",) * n, vmem_limit_bytes=VMEM
    )
    sizes = dict(block=block, extent=extent, intervals=intervals)

    hartley = hartley_table(extent)
    high = lax.reduce_precision(hartley, 8, 7)
    tables = (high.astype(jnp.bfloat16), (hartley - high).astype(jnp.bfloat16))

    step = 4
    table_spec = pl.BlockSpec((extent, extent), lambda a: (0, 0))
    plane_spec = pl.BlockSpec((step, extent, extent), lambda a: (a, 0, 0))
    part_spec = pl.BlockSpec((groups, step, part, extent), lambda a: (0, a, 0, 0))
    part_shape = jax.ShapeDtypeStruct((groups, planes, part, extent), f32)

    def forward(field, other=None):
        choose = other is not None
        last = (lax.axis_index("tm") == intervals - 1).astype(jnp.int32).reshape(1)
        extra = [pl.BlockSpec(memory_space=pltpu.SMEM)] if choose else []
        return pl.pallas_call(
            lambda *r: forward_kernel(*r, choose=choose, chunks=chunks),
            grid=(planes // step,),
            in_specs=extra + [plane_spec] * (1 + choose) + [table_spec] * 2,
            out_specs=[part_spec] * chunks,
            out_shape=[part_shape] * chunks,
            compiler_params=params(1),
            name="forward",
        )(*([last] if choose else []), field, *([other] if choose else []), *tables)

    def inverse(parts):
        return pl.pallas_call(
            inverse_kernel,
            grid=(planes // step,),
            in_specs=[part_spec] * chunks + [table_spec] * 2,
            out_specs=plane_spec,
            out_shape=jax.ShapeDtypeStruct((planes, extent, extent), f32),
            compiler_params=params(1),
            name="inverse",
        )(*parts, *tables)

    def exchange(x):
        return lax.all_to_all(x, ("tm", "core"), split_axis=0, concat_axis=0, tiled=True)

    def line_gather(x):
        return lax.all_gather(x, "line", axis=0)

    sent_states = forward(states[0])
    sent_sources = forward(forcing[0], inflow)

    group = lax.axis_index("tm") * cores + lax.axis_index("core")
    place = lax.axis_index("line").astype(jnp.int32).reshape(1)
    wavenumber = group * rows + jnp.arange(rows, dtype=jnp.int32)
    mu = (
        lattice_symbol(wavenumber, extent)[:, None]
        + lattice_symbol(jnp.arange(extent, dtype=jnp.int32), extent)[None, :]
    )
    ncoef = coef_count(intervals)
    coefs = pl.pallas_call(
        lambda *r: coef_kernel(*r, **sizes),
        grid=(rows // SUB, extent // LANE),
        in_specs=[
            pl.BlockSpec(memory_space=pltpu.SMEM),
            pl.BlockSpec((SUB, LANE), lambda r, l: (r, l)),
        ],
        out_specs=pl.BlockSpec((ncoef, SUB, LANE), lambda r, l: (0, r, l)),
        out_shape=jax.ShapeDtypeStruct((ncoef, rows, extent), f32),
        compiler_params=params(2),
        name="coefs",
    )(timestep, mu)

    grid2 = (part // SUB, extent // LANE)
    whole = (intervals, block, part, extent)
    smem = pl.BlockSpec(memory_space=pltpu.SMEM)

    def one_spec(pick):
        return pl.BlockSpec((1, block, SUB, LANE), lambda r, l, t: (pick(t), 0, r, l))

    all_spec = pl.BlockSpec((intervals, block, SUB, LANE), lambda r, l: (0, 0, r, l))
    before = lambda t: lax.rem(t + intervals - 1, intervals)
    same = lambda t: t
    ncoarse = (intervals - 1) * (intervals - 2) // 2

    defect_parts = []
    state_parts = []
    for i in range(chunks):
        first = i * part // SUB
        coef3 = pl.BlockSpec((ncoef, SUB, LANE), lambda r, l, t: (0, first + r, l))
        coef2 = pl.BlockSpec((ncoef, SUB, LANE), lambda r, l: (0, first + r, l))
        s = exchange(sent_states[i]).reshape(whole)
        f = exchange(sent_sources[i]).reshape(whole)
        ends = pl.pallas_call(
            lambda *r: advance_ends_kernel(*r, **sizes),
            grid=grid2 + (intervals - 1,),
            in_specs=[coef3, one_spec(same), one_spec(same)],
            out_specs=pl.BlockSpec((2, 1, FINE, SUB, LANE), lambda r, l, t: (0, t, 0, r, l)),
            out_shape=jax.ShapeDtypeStruct((2, intervals - 1, FINE, part, extent), f32),
            compiler_params=params(3),
            name="advance_ends",
        )(coefs, s, f)
        ends = line_gather(ends)
        relaxed, error, ends = pl.pallas_call(
            lambda *r: relax_kernel(*r, **sizes),
            grid=grid2 + (intervals,),
            in_specs=[
                smem,
                coef3,
                one_spec(before),
                one_spec(before),
                one_spec(same),
                pl.BlockSpec(
                    (count, 2, 1, FINE, SUB, LANE),
                    lambda r, l, t: (0, 0, jnp.maximum(t - 1, 0), 0, r, l),
                ),
            ],
            out_specs=[
                one_spec(same),
                one_spec(same),
                pl.BlockSpec((2, 1, FINE, SUB, LANE), lambda r, l, t: (0, t, 0, r, l)),
            ],
            out_shape=[
                jax.ShapeDtypeStruct(whole, f32),
                jax.ShapeDtypeStruct(whole, f32),
                jax.ShapeDtypeStruct((2, intervals, FINE, part, extent), f32),
            ],
            compiler_params=params(3),
            name="relax",
        )(place, coefs, s, f, s, ends)
        ends = line_gather(ends)
        defect, ends = pl.pallas_call(
            lambda *r: defect_kernel(*r, **sizes),
            grid=grid2,
            in_specs=[
                smem,
                coef2,
                all_spec,
                pl.BlockSpec(
                    (count, 2, intervals, FINE, SUB, LANE), lambda r, l: (0, 0, 0, 0, r, l)
                ),
            ],
            out_specs=[
                all_spec,
                pl.BlockSpec((2, ncoarse, SUB, LANE), lambda r, l: (0, 0, r, l)),
            ],
            out_shape=[
                jax.ShapeDtypeStruct(whole, f32),
                jax.ShapeDtypeStruct((2, ncoarse, part, extent), f32),
            ],
            compiler_params=params(2),
            name="defect",
        )(place, coefs, error, ends)
        defect_parts.append(exchange(defect.reshape(part_shape.shape)))
        ends = line_gather(ends)
        updated = pl.pallas_call(
            lambda *r: correct_kernel(*r, **sizes),
            grid=grid2,
            in_specs=[
                smem,
                coef2,
                all_spec,
                all_spec,
                pl.BlockSpec((count, 2, ncoarse, SUB, LANE), lambda r, l: (0, 0, 0, r, l)),
            ],
            out_specs=all_spec,
            out_shape=jax.ShapeDtypeStruct(whole, f32),
            compiler_params=params(2),
            name="correct",
        )(place, coefs, relaxed, defect, ends)
        state_parts.append(exchange(updated.reshape(part_shape.shape)))
    return inverse(state_parts)[None], inverse(defect_parts)[None]


def solution(mesh):
    intervals, spaces = mesh.shape["tm"], mesh.shape["space"]
    cores = 2
    inner = Mesh(
        mesh.devices.reshape(intervals, spaces // cores, cores), ("tm", "line", "core")
    )
    field = P("tm", ("line", "core"), None, None)
    return jax.shard_map(
        on_device,
        mesh=inner,
        in_specs=(field, field, P(("line", "core"), None, None), P()),
        out_specs=(field, field),
        check_vma=False,
    )
```
